32 devices in a mesh: comp: 2 (over core), blk: 16 (over z, y, x).
Axes of the slice: x: 2, y: 2, z: 4, core: 2. Of those that a mesh axis runs over, the one named last changes fastest.
Arguments:
- initial: float32 [2, 5, 128, 2048], P('comp', None, 'blk'), may hold values from -3 to 3
- ice_forcing: float32 [5, 128, 2048], P(None, 'blk'), may hold values from -2 to 4, as said below
- ocean_current: float32 [2, 128, 2048], P(None, 'blk'), may hold values from -1 to 1
- ice_cover: int32 [128, 2048], P('blk'), may hold values from 0 to 1, as said below
- targets: int32 [2, 128, 2048], P(None, 'blk'), may hold values from 0 to 32767, as said below
- weights: int32 [2, 128, 2048], P(None, 'blk'), may hold values from 1 to 4
Outputs:
- state_out: float32 [2, 5, 128, 2048], P('comp', None, 'blk')
- coupled: float32 [2, 3, 128, 2048], P('comp', None, 'blk')
The draws below stay inside these ranges and needn't reach their ends.
Inputs may be any that keep to these rules, and one draw needn't show every extreme that they name: `ice_forcing`: channel 0 (mass) lies in 0.5 to 4, channel 1 (strength) and channel 4 (melt rate) in 0.2 to 2, channels 2 and 3 (wind stress) in -2 to 2. `ice_cover`: the share of ice-covered cells differs from strip to strip of 8 rows. `targets`: an entry of an ice cell at row r of its strip names an ocean row of the window no earlier than r.
All inputs are finite; a program needn't handle non-finite values.
Results may differ from the reference program's by a relative error of at most 0.0003.
Values sent between devices are 32-bit elements; how exact they have to be, the bound alone decides.
A program may use at most 128 MiB of HBM per device.

```python
import math
import jax
import jax.numpy as jnp
from jax import lax

CX = 8
NY = 2048
SUBCYCLES = 16
INTERSECTIONS = 2
NX = 128


def smooth_field(key, channels):
    row_pos = jnp.arange(NX, dtype=jnp.float32)[None, :, None]
    col_pos = jnp.arange(NY, dtype=jnp.float32)[None, None, :]
    summed = jnp.zeros((channels, NX, NY), jnp.float32)
    for wave_index in range(3):
        wave_key = jax.random.fold_in(key, 100 + wave_index)
        picks = jax.random.uniform(wave_key, (3, channels), jnp.float32)
        row_length = jnp.exp(math.log(48.0) + (math.log(160.0) - math.log(48.0)) * picks[0])[:, None, None]
        col_length = jnp.exp(math.log(32.0) + (math.log(512.0) - math.log(32.0)) * picks[1])[:, None, None]
        summed = summed + jnp.sin(2.0 * math.pi * (row_pos / row_length + col_pos / col_length + picks[2][:, None, None]))
    return summed / 2.0


def draw_initial(key, part):
    smooth = smooth_field(jax.random.fold_in(key, 31), 10).reshape(2, 5, NX, NY)
    noise = jax.random.normal(jax.random.fold_in(key, 32), (2, 5, NX, NY), jnp.float32)
    values = 0.8 * smooth + 0.35 * noise
    return jnp.clip(values, -3.0, 3.0).astype(jnp.float32)


def draw_ice_forcing(key, part):
    shape = (NX, NY)
    keys = jax.random.split(key, 5)
    smooth = smooth_field(jax.random.fold_in(key, 51), 2)
    mass = jnp.exp(jax.random.uniform(keys[0], shape, jnp.float32, math.log(0.5), math.log(4.0)))
    strength = jnp.exp(jax.random.uniform(keys[1], shape, jnp.float32, math.log(0.2), math.log(2.0)))
    wind_x = jnp.clip(0.6 * smooth[0] + 0.3 * jax.random.normal(keys[2], shape, jnp.float32), -2.0, 2.0)
    wind_y = jnp.clip(0.6 * smooth[1] + 0.3 * jax.random.normal(keys[3], shape, jnp.float32), -2.0, 2.0)
    melt = jnp.exp(jax.random.uniform(keys[4], shape, jnp.float32, math.log(0.2), math.log(2.0)))
    return jnp.stack([mass, strength, wind_x, wind_y, melt]).astype(jnp.float32)


def draw_ocean_current(key, part):
    smooth = smooth_field(jax.random.fold_in(key, 41), 2)
    noise = jax.random.uniform(jax.random.fold_in(key, 42), (2, NX, NY), jnp.float32, -1.0, 1.0)
    along = 0.6 * jnp.tanh(3.0 * smooth[0]) + 0.35 * noise[0]
    sideways = 0.5 * smooth[1] + 0.4 * noise[1]
    return jnp.clip(jnp.stack([along, sideways]), -1.0, 1.0).astype(jnp.float32)


def draw_ice_cover(key, part):
    level = jnp.minimum(jax.random.randint(jax.random.fold_in(key, 11), (NX // CX,), 0, 24), 8)
    cells = jax.random.randint(jax.random.fold_in(key, 12), (NX, NY), 0, 8)
    strip = jnp.arange(NX, dtype=jnp.int32) // CX
    return (cells < level[strip][:, None]).astype(jnp.int32)


def draw_targets(key, part):
    offset = jax.random.randint(jax.random.fold_in(key, 21), (INTERSECTIONS, NX, NY), 0, CX + 1)
    jitter = jax.random.randint(jax.random.fold_in(key, 22), (INTERSECTIONS, NX, NY), -2, 3)
    local_row = (jnp.arange(NX, dtype=jnp.int32) % CX)[None, :, None]
    column = jnp.arange(NY, dtype=jnp.int32)[None, None, :]
    return ((local_row + offset) * NY + (column + jitter) % NY).astype(jnp.int32)


def with_ends(array, stream_key, least, high):
    place = [jax.random.randint(jax.random.fold_in(stream_key, axis), (), 0, length) for axis, length in enumerate(array.shape)]
    main_axis = array.shape.index(max(array.shape))
    beside = place[:main_axis] + [(place[main_axis] + 1) % array.shape[main_axis]] + place[main_axis + 1:]
    return array.at[tuple(place)].set(least).at[tuple(beside)].set(high)


def setup_inputs(seed: int = 0) -> dict:
    key_list = jax.random.split(jax.random.key(seed), 7)
    initial = draw_initial(jax.random.fold_in(key_list[6], 71), 0)
    ice_forcing = draw_ice_forcing(jax.random.fold_in(key_list[6], 71), 0)
    ocean_current = draw_ocean_current(jax.random.fold_in(key_list[6], 71), 0)
    ice_cover = draw_ice_cover(jax.random.fold_in(key_list[6], 71), 0)
    targets = draw_targets(jax.random.fold_in(key_list[6], 71), 0)
    weights = with_ends(jax.random.randint(key_list[5], (INTERSECTIONS, NX, NY), 1, 5), jax.random.fold_in(key_list[5], 1), 1, 4).astype(jnp.int32)
    return dict(initial=initial, ice_forcing=ice_forcing, ocean_current=ocean_current, ice_cover=ice_cover, targets=targets, weights=weights)


relax_rate = 0.5
ecc_sq = 4.0
delta_floor = 0.1
coriolis = 0.1
drag_coef = 1.0
inertia = 4.0
courant = 0.2
dilution = 0.5
weight_norm = 4.0
level_speed = (1.0, 0.8, 0.6, 0.45, 0.3)

def along_rows(field):
    return 0.5 * (field[..., 2:, :] - field[..., :-2, :])

def across(field):
    padded = jnp.pad(field, [(0, 0)] * (field.ndim - 1) + [(1, 1)])
    return 0.5 * (padded[..., 2:] - padded[..., :-2])

def ice_step(fields, forcing, current, covered):
    vel_x = fields[0]
    vel_y = fields[1]
    strain_d = along_rows(vel_x) + across(vel_y[1:-1])
    strain_t = along_rows(vel_x) - across(vel_y[1:-1])
    strain_s = across(vel_x[1:-1]) + along_rows(vel_y)
    delta = jnp.sqrt(strain_d * strain_d + (strain_t * strain_t + strain_s * strain_s) / ecc_sq + delta_floor * delta_floor)
    press = forcing[1, 1:-1] * covered[1:-1]
    sig_one = (fields[2, 1:-1] + relax_rate * press * (strain_d / delta - 1.0)) / (1.0 + relax_rate)
    sig_two = (fields[3, 1:-1] + relax_rate * press * strain_t / (ecc_sq * delta)) / (1.0 + relax_rate)
    sig_shear = (fields[4, 1:-1] + relax_rate * press * strain_s / (2.0 * ecc_sq * delta)) / (1.0 + relax_rate)
    sig_xx = 0.5 * (sig_one + sig_two)
    sig_yy = 0.5 * (sig_one - sig_two)
    force_x = along_rows(sig_xx) + across(sig_shear[1:-1])
    force_y = along_rows(sig_shear) + across(sig_yy[1:-1])
    beta = inertia * forcing[0, 2:-2]
    old_x = vel_x[2:-2]
    old_y = vel_y[2:-2]
    denom = beta + drag_coef
    new_x = covered[2:-2] * (beta * old_x + coriolis * beta * old_y + force_x + forcing[2, 2:-2] + drag_coef * current[0, 2:-2]) / denom
    new_y = covered[2:-2] * (beta * old_y - coriolis * beta * old_x + force_y + forcing[3, 2:-2] + drag_coef * current[1, 2:-2]) / denom
    return jnp.stack([new_x, new_y, sig_one[1:-1], sig_two[1:-1], sig_shear[1:-1]])

def ocean_step(tracer, current):
    speed = jnp.asarray(level_speed, jnp.float32)[:, None, None]
    centre = tracer[:, 2:-2]
    below = centre - tracer[:, 1:-3]
    above = tracer[:, 3:-1] - centre
    padded = jnp.pad(centre, ((0, 0), (0, 0), (1, 1)))
    left_diff = centre - padded[:, :, :-2]
    right_diff = padded[:, :, 2:] - centre
    speed_x = speed * current[0, 2:-2][None]
    speed_y = speed * current[1, 2:-2][None]
    change = jnp.maximum(speed_x, 0.0) * below + jnp.minimum(speed_x, 0.0) * above + jnp.maximum(speed_y, 0.0) * left_diff + jnp.minimum(speed_y, 0.0) * right_diff
    return centre - courant * change

def coupling_terms(fields, forcing, current, covered):
    stress_x = covered * drag_coef * (fields[0] - current[0])
    stress_y = covered * drag_coef * (fields[1] - current[1])
    fresh = forcing[4] * covered * jnp.sqrt(1.0 + fields[0] * fields[0] + fields[1] * fields[1])
    return jnp.stack([stress_x, stress_y, fresh])

def pad_rows(values):
    return jnp.pad(values, [(0, 0)] * (values.ndim - 2) + [(2, 2), (0, 0)])

def reference(initial, ice_forcing, ocean_current, ice_cover, targets, weights):
    covered = ice_cover.astype(jnp.float32)
    forcing_pad = pad_rows(ice_forcing)
    current_pad = pad_rows(ocean_current)
    cover_pad = pad_rows(covered)

    def one_turn(carry, unused):
        ice_fields, salinity, total = carry
        ice_fields = ice_step(pad_rows(ice_fields), forcing_pad, current_pad, cover_pad)
        salinity = ocean_step(pad_rows(salinity), current_pad)
        total = total + coupling_terms(ice_fields, ice_forcing, ocean_current, covered)
        return ((ice_fields, salinity, total), None)
    start = (initial[0], initial[1], jnp.zeros((3, NX, NY), jnp.float32))
    (ice_fields, salinity, total), unused = lax.scan(one_turn, start, None, length=SUBCYCLES)
    average = total / SUBCYCLES
    row_index = jnp.arange(NX, dtype=jnp.int32)[:, None]
    base = row_index // CX * (CX * NY)
    glob = (targets + base[None]) % (NX * NY)
    scaled = weights.astype(jnp.float32) / weight_norm
    flat_glob = glob.reshape(-1)

    def spread(single):
        return jax.ops.segment_sum((single[None] * scaled).reshape(-1), flat_glob, num_segments=NX * NY)
    flux = jax.vmap(spread)(average).reshape(3, NX, NY)
    salinity = jnp.concatenate([salinity[:1] - dilution * flux[2][None], salinity[1:]], axis=0)
    state_out = jnp.stack([ice_fields, salinity])
    coupled = jnp.stack([average, flux])
    return (state_out, coupled)
```

```python
import functools

import jax
import jax.numpy as jnp
from jax import lax
from jax.experimental import pallas as pl
from jax.experimental.pallas import tpu as pltpu
from jax.sharding import PartitionSpec as P

SUBCYCLES = 16
MESH = pl.DeviceIdType.MESH
PAD = 128

coriolis = 0.1
inertia = 4.0
courant = 0.2
dilution = 0.5
weight_norm = 4.0
level_speed = (1.0, 0.8, 0.6, 0.45, 0.3)


def rolled(value, steps, axis):
    return pltpu.roll(value, steps % value.shape[axis], axis)


def rows_diff(value):
    return rolled(value, -1, 0) - rolled(value, 1, 0)


def chunk_width(cols):
    return 256 if cols % 256 == 0 else 128


def stress_stage(work, stat, start, width):
    wide = pl.ds(start, width + 2 * PAD)
    mid = pl.ds(start + PAD, width)
    inner = slice(PAD, PAD + width)
    vel_x, vel_y = work[0, :, wide], work[1, :, wide]
    cx = (rolled(vel_x, -1, 1) - rolled(vel_x, 1, 1))[:, inner]
    cy = (rolled(vel_y, -1, 1) - rolled(vel_y, 1, 1))[:, inner]
    rx = rows_diff(vel_x[:, inner])
    ry = rows_diff(vel_y[:, inner])
    e_d = rx + cy
    e_t = rx - cy
    e_s = cx + ry
    inv = lax.rsqrt(0.25 * (e_d * e_d) + 0.0625 * (e_t * e_t + e_s * e_s) + 0.01)
    third = stat[0, :, pl.ds(start, width)]
    scaled = third * inv
    work[2, :, mid] = work[2, :, mid] * (2.0 / 3.0) + (0.5 * scaled * e_d - third)
    work[3, :, mid] = work[3, :, mid] * (2.0 / 3.0) + 0.125 * scaled * e_t
    work[4, :, mid] = work[4, :, mid] * (2.0 / 3.0) + 0.0625 * scaled * e_s


def velocity_stage(work, stat, total, start, width, rows):
    wide = pl.ds(start, width + 2 * PAD)
    mid = pl.ds(start + PAD, width)
    here = pl.ds(start, width)
    inner = slice(PAD, PAD + width)
    shear = work[4, :, wide]
    one, two = work[2, :, wide], work[3, :, wide]
    across_shear = (rolled(shear, -1, 1) - rolled(shear, 1, 1))[:, inner]
    lower = one - two
    across_yy = (rolled(lower, -1, 1) - rolled(lower, 1, 1))[:, inner]
    force_x = rows_diff((one + two)[:, inner]) + 2.0 * across_shear
    force_y = 2.0 * rows_diff(shear[:, inner]) + across_yy
    old_x, old_y = work[0, :, mid], work[1, :, mid]
    keep, push = stat[1, :, here], stat[2, :, here]
    new_x = keep * (old_x + coriolis * old_y) + push * force_x + stat[3, :, here]
    new_y = keep * (old_y - coriolis * old_x) + push * force_y + stat[4, :, here]
    work[0, :, mid] = new_x
    work[1, :, mid] = new_y
    own_x, own_y = new_x[rows : 2 * rows], new_y[rows : 2 * rows]
    total[0, :, here] += own_x
    total[1, :, here] += own_y
    total[2, :, here] += jnp.sqrt(1.0 + own_x * own_x + own_y * own_y)


def ocean_stage(source, target, coef, start, width):
    wide = pl.ds(start, width + 2 * PAD)
    mid = pl.ds(start + PAD, width)
    here = pl.ds(start, width)
    inner = slice(PAD, PAD + width)
    up, down, east, west = (coef[i, :, here] for i in range(4))
    for level, speed in enumerate(level_speed):
        tracer = source[level, :, wide]
        centre = tracer[:, inner]
        right = rolled(tracer, -1, 1)[:, inner] - centre
        left = centre - rolled(tracer, 1, 1)[:, inner]
        above = rolled(centre, -1, 0) - centre
        below = centre - rolled(centre, 1, 0)
        change = up * below + down * above + east * left + west * right
        target[level, :, mid] = centre - speed * change


def turns_kernel(
    initial, forcing, current, cover, state, average,
    own, own_stat, halo, halo_stat, work, spare, stat, total, mean,
    send, recv, stat_send, stat_recv, mean_send, mean_recv,
):
    me = lax.axis_index("blk")
    comp = lax.axis_index("comp")
    count = lax.axis_size("blk")
    fields, rows, cols = initial.shape
    width = chunk_width(cols)
    chunks = cols // width
    right, left = lax.rem(me + 1, count), lax.rem(me + count - 1, count)
    has_left, has_right = me > 0, me < count - 1

    barrier = pltpu.get_barrier_semaphore()
    pl.semaphore_signal(barrier, inc=1, device_id={"blk": right}, device_id_type=MESH)
    pl.semaphore_signal(barrier, inc=1, device_id={"blk": left}, device_id_type=MESH)
    pl.semaphore_signal(barrier, inc=1, device_id={"comp": 1 - comp}, device_id_type=MESH)

    work[...] = jnp.zeros_like(work)
    spare[...] = jnp.zeros_like(spare)
    total[...] = jnp.zeros_like(total)
    covered = cover[...].astype(jnp.float32)

    def copies(source, target, out_sem, in_sem):
        up = pltpu.make_async_remote_copy(
            source, target.at[0], out_sem.at[0], in_sem.at[0],
            device_id={"blk": right}, device_id_type=MESH,
        )
        down = pltpu.make_async_remote_copy(
            source, target.at[1], out_sem.at[1], in_sem.at[1],
            device_id={"blk": left}, device_id_type=MESH,
        )
        return up, down

    def start(pair):
        pl.when(has_right)(pair[0].start)
        pl.when(has_left)(pair[1].start)

    def arrive(pair):
        pl.when(has_left)(pair[0].wait_recv)
        pl.when(has_right)(pair[1].wait_recv)

    def sent(pair):
        pl.when(has_right)(pair[0].wait_send)
        pl.when(has_left)(pair[1].wait_send)

    def clear_edges(turns):
        @pl.when(jnp.logical_not(has_left))
        def _():
            halo_stat[0] = jnp.zeros_like(halo_stat[0])
            for turn in range(turns):
                halo[turn, 0] = jnp.zeros_like(halo[turn, 0])

        @pl.when(jnp.logical_not(has_right))
        def _():
            halo_stat[1] = jnp.zeros_like(halo_stat[1])
            for turn in range(turns):
                halo[turn, 1] = jnp.zeros_like(halo[turn, 1])

    inside = slice(PAD, PAD + cols)

    def fill(turn, source):
        for field in range(fields):
            work[field, 0:rows, inside] = halo[turn, 0, field]
            work[field, rows : 2 * rows, inside] = source[field]
            work[field, 2 * rows : 3 * rows, inside] = halo[turn, 1, field]

    mean_copy = pltpu.make_async_remote_copy(
        mean, average, mean_send, mean_recv,
        device_id={"comp": 1 - comp}, device_id_type=MESH,
    )

    @pl.when(comp == 0)
    def _():
        depth = rows // 2
        turns = SUBCYCLES // depth
        clear_edges(turns)
        push = covered / (inertia * forcing[0] + 1.0)
        own_stat[0] = forcing[1] * covered * (1.0 / 3.0)
        own_stat[1] = push
        own_stat[2] = push * (forcing[2] + current[0])
        own_stat[3] = push * (forcing[3] + current[1])
        pl.semaphore_wait(barrier, 3)
        stat_pair = copies(own_stat, halo_stat, stat_send, stat_recv)
        start(stat_pair)
        pairs = []
        for turn in range(turns):
            source = initial if turn == 0 else own.at[turn - 1]
            pair = copies(source, halo.at[turn], send.at[turn], recv.at[turn])
            pairs.append(pair)
            start(pair)
            if turn == 0:
                arrive(stat_pair)
                for place, block in enumerate((halo_stat.at[0], own_stat, halo_stat.at[1])):
                    span = slice(place * rows, (place + 1) * rows)
                    push = block[1]
                    stat[0, span] = block[0]
                    stat[1, span] = jnp.where(push > 0.0, 1.0 - push, 0.0)
                    stat[2, span] = 0.25 * push
                    stat[3, span] = block[2]
                    stat[4, span] = block[3]
            arrive(pair)
            fill(turn, source)

            def subcycle(step, carry):
                for chunk in range(chunks):
                    stress_stage(work, stat, chunk * width, width)
                for chunk in range(chunks):
                    velocity_stage(work, stat, total, chunk * width, width, rows)
                return carry

            lax.fori_loop(0, depth, subcycle, 0)
            final = state if turn == turns - 1 else own.at[turn]
            for field in range(fields):
                final[field] = work[field, rows : 2 * rows, inside]
        share = 1.0 / SUBCYCLES
        mean[0] = total[0] * share - covered * current[0]
        mean[1] = total[1] * share - covered * current[1]
        mean[2] = forcing[4] * covered * (total[2] * share)
        mean_copy.start()
        average[...] = mean[...]
        sent(stat_pair)
        for pair in pairs:
            sent(pair)
        mean_copy.wait_send()

    @pl.when(comp == 1)
    def _():
        depth = rows
        turns = SUBCYCLES // depth
        clear_edges(turns)
        pl.semaphore_wait(barrier, 3)
        stat_pair = copies(current, halo_stat.at[:, pl.ds(0, 2)], stat_send, stat_recv)
        start(stat_pair)
        pairs = []
        for turn in range(turns):
            source = initial if turn == 0 else own.at[turn - 1]
            pair = copies(source, halo.at[turn], send.at[turn], recv.at[turn])
            pairs.append(pair)
            start(pair)
            if turn == 0:
                arrive(stat_pair)
                for place in range(3):
                    span = slice(place * rows, (place + 1) * rows)
                    for axis in range(2):
                        if place == 1:
                            speed = current[axis]
                        else:
                            speed = halo_stat[place // 2, axis]
                        stat[2 * axis, span] = courant * jnp.maximum(speed, 0.0)
                        stat[2 * axis + 1, span] = courant * jnp.minimum(speed, 0.0)
            arrive(pair)
            fill(turn, source)

            def substeps(step, carry):
                for chunk in range(chunks):
                    ocean_stage(work, spare, stat, chunk * width, width)
                for chunk in range(chunks):
                    ocean_stage(spare, work, stat, chunk * width, width)
                return carry

            lax.fori_loop(0, depth // 2, substeps, 0)
            final = state if turn == turns - 1 else own.at[turn]
            for field in range(fields):
                final[field] = work[field, rows : 2 * rows, inside]
        sent(stat_pair)
        for pair in pairs:
            sent(pair)
        mean_copy.wait_recv()


def run_turns(initial, forcing, current, cover):
    fields, rows, cols = initial.shape
    most = SUBCYCLES // (rows // 2)
    f32 = jnp.float32
    vmem = pl.BlockSpec(memory_space=pltpu.VMEM)
    dma = pltpu.SemaphoreType.DMA
    return pl.pallas_call(
        turns_kernel,
        out_shape=(
            jax.ShapeDtypeStruct((fields, rows, cols), f32),
            jax.ShapeDtypeStruct((3, rows, cols), f32),
        ),
        in_specs=[vmem] * 4,
        out_specs=(vmem, vmem),
        scratch_shapes=[
            pltpu.VMEM((most, fields, rows, cols), f32),
            pltpu.VMEM((4, rows, cols), f32),
            pltpu.VMEM((most, 2, fields, rows, cols), f32),
            pltpu.VMEM((2, 4, rows, cols), f32),
            pltpu.VMEM((fields, 3 * rows, cols + 2 * PAD), f32),
            pltpu.VMEM((fields, 3 * rows, cols + 2 * PAD), f32),
            pltpu.VMEM((5, 3 * rows, cols), f32),
            pltpu.VMEM((3, rows, cols), f32),
            pltpu.VMEM((3, rows, cols), f32),
            dma((most, 2)), dma((most, 2)), dma((2,)), dma((2,)), dma, dma,
        ],
        compiler_params=pltpu.CompilerParams(
            collective_id=0, has_side_effects=True, vmem_limit_bytes=40 * 1024 * 1024
        ),
        name="turns",
    )(initial, forcing, current, cover)


def remap_kernel(average, targets, weights, window, acc, low_index, high_index):
    comp = lax.axis_index("comp")
    channels, rows, cols = average.shape
    span = low_index.shape[1]
    low_count, high_count = low_index.shape[0], high_index.shape[0]
    bf16 = jnp.bfloat16
    blocks = cols // low_count
    low_index[...] = lax.broadcasted_iota(jnp.int32, low_index.shape, 0).astype(bf16)
    high_index[...] = lax.broadcasted_iota(jnp.int32, high_index.shape, 0).astype(bf16)
    acc[...] = jnp.zeros_like(acc)

    def one_row(row, carry):
        for piece in range(cols // span):
            place = pl.ds(piece * span, span)
            target = targets[comp, pl.ds(row, 1), place]
            scale = weights[comp, pl.ds(row, 1), place].astype(jnp.float32) * (1.0 / weight_norm)
            low = lax.rem(target, low_count)
            block = lax.rem(lax.div(target, low_count), blocks)
            line = lax.div(target, cols)
            high = (lax.div(line, rows) * blocks + block) * rows + lax.rem(line, rows)
            low_hot = jnp.where(low_index[...] == low.astype(bf16), bf16(1), bf16(0))
            match = high_index[...] == high.astype(bf16)
            parts = []
            for channel in range(channels):
                value = average[channel, pl.ds(row, 1), place] * scale
                coarse = value.astype(bf16)
                fine = (value - coarse.astype(jnp.float32)).astype(bf16)
                parts.append(jnp.where(match, coarse, bf16(0)))
                parts.append(jnp.where(match, fine, bf16(0)))
            spread = jnp.concatenate(parts, axis=0)
            acc[...] += lax.dot_general(
                spread, low_hot, (((1,), (1,)), ((), ())), preferred_element_type=jnp.float32
            )
        return carry

    lax.fori_loop(0, rows, one_row, 0)
    for channel in range(channels):
        for half in range(2):
            for block in range(blocks):
                base = 2 * channel * high_count + (half * blocks + block) * rows
                window[channel, half, :, block * low_count : (block + 1) * low_count] = (
                    acc[base : base + rows] + acc[base + high_count : base + high_count + rows]
                )


def run_remap(average, targets, weights):
    channels, rows, cols = average.shape
    low_count = 256 if cols % 256 == 0 else 128
    high_count = 2 * rows * cols // low_count
    span = min(1024, cols)
    vmem = pl.BlockSpec(memory_space=pltpu.VMEM)
    return pl.pallas_call(
        remap_kernel,
        out_shape=jax.ShapeDtypeStruct((channels, 2, rows, cols), jnp.float32),
        in_specs=[vmem] * 3,
        out_specs=vmem,
        scratch_shapes=[
            pltpu.VMEM((2 * channels * high_count, low_count), jnp.float32),
            pltpu.VMEM((low_count, span), jnp.bfloat16),
            pltpu.VMEM((high_count, span), jnp.bfloat16),
        ],
        compiler_params=pltpu.CompilerParams(vmem_limit_bytes=40 * 1024 * 1024),
        name="remap",
    )(average, targets, weights)


def join_kernel(
    window, state, average, out_state, out_pair, beside, carry, before,
    side_send, side_recv, next_send, next_recv,
):
    me = lax.axis_index("blk")
    comp = lax.axis_index("comp")
    count = lax.axis_size("blk")
    right, left = lax.rem(me + 1, count), lax.rem(me + count - 1, count)
    barrier = pltpu.get_barrier_semaphore()
    pl.semaphore_signal(barrier, inc=1, device_id={"blk": right}, device_id_type=MESH)
    pl.semaphore_signal(barrier, inc=1, device_id={"blk": left}, device_id_type=MESH)
    pl.semaphore_signal(barrier, inc=1, device_id={"comp": 1 - comp}, device_id_type=MESH)
    pl.semaphore_wait(barrier, 3)
    side = pltpu.make_async_remote_copy(
        window, beside, side_send, side_recv,
        device_id={"comp": 1 - comp}, device_id_type=MESH,
    )
    onward = pltpu.make_async_remote_copy(
        carry, before, next_send, next_recv, device_id={"blk": right}, device_id_type=MESH
    )

    @pl.when(comp == 0)
    def _():
        side.start()
        out_state[...] = state[...]
        out_pair[...] = average[...]
        side.wait_send()

    @pl.when(comp == 1)
    def _():
        side.wait_recv()
        carry[...] = window[:, 1] + beside[:, 1]
        onward.start()
        out_pair[...] = window[:, 0] + beside[:, 0]
        out_state[...] = state[...]
        onward.wait_recv()
        out_pair[...] += before[...]
        out_state[0] -= dilution * out_pair[2]
        onward.wait_send()


def run_join(window, state, average):
    channels, rows, cols = average.shape
    vmem = pl.BlockSpec(memory_space=pltpu.VMEM)
    dma = pltpu.SemaphoreType.DMA
    return pl.pallas_call(
        join_kernel,
        out_shape=(
            jax.ShapeDtypeStruct(state.shape, jnp.float32),
            jax.ShapeDtypeStruct(average.shape, jnp.float32),
        ),
        in_specs=[vmem] * 3,
        out_specs=(vmem, vmem),
        scratch_shapes=[
            pltpu.VMEM(window.shape, jnp.float32),
            pltpu.VMEM(average.shape, jnp.float32),
            pltpu.VMEM(average.shape, jnp.float32),
            dma, dma, dma, dma,
        ],
        compiler_params=pltpu.CompilerParams(
            collective_id=1, has_side_effects=True, vmem_limit_bytes=40 * 1024 * 1024
        ),
        name="join",
    )(window, state, average)


def body(initial, ice_forcing, ocean_current, ice_cover, targets, weights):
    state, average = run_turns(initial[0], ice_forcing, ocean_current, ice_cover)
    window = run_remap(average, targets, weights)
    state, coupled = run_join(window, state, average)
    return (state[None], coupled[None])


def solution(mesh):
    placed = (
        P("comp", None, "blk", None),
        P(None, "blk", None),
        P(None, "blk", None),
        P("blk", None),
        P(None, "blk", None),
        P(None, "blk", None),
    )
    return jax.shard_map(
        body,
        mesh=mesh,
        in_specs=placed,
        out_specs=(P("comp", None, "blk", None), P("comp", None, "blk", None)),
        check_vma=False,
    )
```

```python
import functools

import jax
import jax.numpy as jnp
from jax import lax
from jax.experimental import pallas as pl
from jax.experimental.pallas import tpu as pltpu
from jax.sharding import PartitionSpec as P

SUBCYCLES = 16
MESH = pl.DeviceIdType.MESH
PAD = 128

coriolis = 0.1
inertia = 4.0
courant = 0.2
dilution = 0.5
weight_norm = 4.0
level_speed = (1.0, 0.8, 0.6, 0.45, 0.3)


def rolled(value, steps, axis):
    return pltpu.roll(value, steps % value.shape[axis], axis)


def rows_diff(value):
    return rolled(value, -1, 0) - rolled(value, 1, 0)


def chunk_width(cols):
    return 256 if cols % 256 == 0 else 128


def stress_stage(work, stat, start, width):
    wide = pl.ds(start, width + 2 * PAD)
    mid = pl.ds(start + PAD, width)
    inner = slice(PAD, PAD + width)
    vel_x, vel_y = work[0, :, wide], work[1, :, wide]
    cx = (rolled(vel_x, -1, 1) - rolled(vel_x, 1, 1))[:, inner]
    cy = (rolled(vel_y, -1, 1) - rolled(vel_y, 1, 1))[:, inner]
    rx = rows_diff(vel_x[:, inner])
    ry = rows_diff(vel_y[:, inner])
    e_d = rx + cy
    e_t = rx - cy
    e_s = cx + ry
    inv = lax.rsqrt(0.25 * (e_d * e_d) + 0.0625 * (e_t * e_t + e_s * e_s) + 0.01)
    third = stat[0, :, pl.ds(start, width)]
    scaled = third * inv
    work[2, :, mid] = work[2, :, mid] * (2.0 / 3.0) + (0.5 * scaled * e_d - third)
    work[3, :, mid] = work[3, :, mid] * (2.0 / 3.0) + 0.125 * scaled * e_t
    work[4, :, mid] = work[4, :, mid] * (2.0 / 3.0) + 0.0625 * scaled * e_s


def velocity_stage(work, stat, total, start, width, rows):
    wide = pl.ds(start, width + 2 * PAD)
    mid = pl.ds(start + PAD, width)
    here = pl.ds(start, width)
    inner = slice(PAD, PAD + width)
    shear = work[4, :, wide]
    one, two = work[2, :, wide], work[3, :, wide]
    across_shear = (rolled(shear, -1, 1) - rolled(shear, 1, 1))[:, inner]
    lower = one - two
    across_yy = (rolled(lower, -1, 1) - rolled(lower, 1, 1))[:, inner]
    force_x = rows_diff((one + two)[:, inner]) + 2.0 * across_shear
    force_y = 2.0 * rows_diff(shear[:, inner]) + across_yy
    old_x, old_y = work[0, :, mid], work[1, :, mid]
    keep, push = stat[1, :, here], stat[2, :, here]
    new_x = keep * (old_x + coriolis * old_y) + push * force_x + stat[3, :, here]
    new_y = keep * (old_y - coriolis * old_x) + push * force_y + stat[4, :, here]
    work[0, :, mid] = new_x
    work[1, :, mid] = new_y
    own_x, own_y = new_x[rows : 2 * rows], new_y[rows : 2 * rows]
    total[0, :, here] += own_x
    total[1, :, here] += own_y
    total[2, :, here] += jnp.sqrt(1.0 + own_x * own_x + own_y * own_y)


def ocean_stage(source, target, coef, start, width):
    wide = pl.ds(start, width + 2 * PAD)
    mid = pl.ds(start + PAD, width)
    here = pl.ds(start, width)
    inner = slice(PAD, PAD + width)
    up, down, east, west = (coef[i, :, here] for i in range(4))
    for level, speed in enumerate(level_speed):
        tracer = source[level, :, wide]
        centre = tracer[:, inner]
        right = rolled(tracer, -1, 1)[:, inner] - centre
        left = centre - rolled(tracer, 1, 1)[:, inner]
        above = rolled(centre, -1, 0) - centre
        below = centre - rolled(centre, 1, 0)
        change = up * below + down * above + east * left + west * right
        target[level, :, mid] = centre - speed * change


def turns_kernel(
    initial_in, forcing_in, current_in, cover_in, state, average,
    initial, forcing, current, cover,
    own, own_stat, halo, halo_stat, work, spare, stat, total, mean,
    load, near_send, near_recv, far_send, far_recv,
    stat_near_send, stat_near_recv, stat_far_send, stat_far_recv,
    mean_send, mean_recv, go,
):
    me = lax.axis_index("blk")
    comp = lax.axis_index("comp")
    count = lax.axis_size("blk")
    fields, rows, cols = initial.shape
    width = chunk_width(cols)
    chunks = cols // width
    near = 1 - lax.rem(me, 2)
    far = 1 - near
    partner = me + 2 * near - 1
    relay_to = me + 4 * near - 2
    relay_from = me - 4 * near + 2
    can_send = jnp.logical_and(relay_to >= 0, relay_to < count)
    can_recv = jnp.logical_and(relay_from >= 0, relay_from < count)
    relay_to = lax.rem(relay_to + count, count)
    relay_from = lax.rem(relay_from + count, count)

    barrier = pltpu.get_barrier_semaphore()

    def greet(where):
        pl.semaphore_signal(barrier, inc=1, device_id=where, device_id_type=MESH)

    greet({"blk": partner})
    greet({"comp": 1 - comp})
    pl.when(can_send)(lambda: greet({"blk": relay_to}))
    pl.when(can_recv)(lambda: greet({"blk": relay_from}))
    loads = [
        pltpu.make_async_copy(source, target, load.at[i])
        for i, (source, target) in enumerate(
            (
                (initial_in, initial),
                (current_in, current),
                (forcing_in, forcing),
                (cover_in, cover),
            )
        )
    ]
    for copy in loads:
        copy.start()

    work[...] = jnp.zeros_like(work)
    total[...] = jnp.zeros_like(total)

    def enter():
        pl.semaphore_wait(barrier, 2 + can_send.astype(jnp.int32) + can_recv.astype(jnp.int32))

    def copies(source, target, pieces, near_sems, far_sems):
        first, second = [], []
        for piece in range(pieces):
            first.append(
                pltpu.make_async_remote_copy(
                    source.at[piece], target.at[far, piece],
                    near_sems[0].at[piece], near_sems[1].at[piece],
                    device_id={"blk": partner}, device_id_type=MESH,
                )
            )
            second.append(
                pltpu.make_async_remote_copy(
                    target.at[near, piece], target.at[far, piece],
                    far_sems[0].at[piece], far_sems[1].at[piece],
                    device_id={"blk": relay_to}, device_id_type=MESH,
                )
            )
        return first, second

    def start(pair):
        for copy in pair[0]:
            copy.start()

    def relay(pair):
        for first, second in zip(*pair):
            first.wait_recv()
            pl.when(can_send)(second.start)

    def arrive(pair):
        @pl.when(can_recv)
        def _():
            for copy in pair[1]:
                copy.wait_recv()

    def sent(pair):
        for copy in pair[0]:
            copy.wait_send()

        @pl.when(can_send)
        def _():
            for copy in pair[1]:
                copy.wait_send()

    def clear_edges(turns):
        @pl.when(jnp.logical_not(can_recv))
        def _():
            halo_stat[far] = jnp.zeros(halo_stat.shape[1:], jnp.float32)
            for turn in range(turns):
                halo[turn, far] = jnp.zeros(halo.shape[2:], jnp.float32)

    inside = slice(PAD, PAD + cols)

    def fill_own(source):
        for field in range(fields):
            work[field, rows : 2 * rows, inside] = source[field]

    def fill_sides(turn):
        for field in range(fields):
            work[field, 0:rows, inside] = halo[turn, 0, field]
            work[field, 2 * rows : 3 * rows, inside] = halo[turn, 1, field]

    def exchange_of(turn, source):
        return copies(
            source, halo.at[turn], fields,
            (near_send.at[turn], near_recv.at[turn]), (far_send.at[turn], far_recv.at[turn]),
        )

    def stats_of(source, pieces):
        return copies(
            source, halo_stat, pieces,
            (stat_near_send, stat_near_recv), (stat_far_send, stat_far_recv),
        )

    mean_copy = pltpu.make_async_remote_copy(
        mean, average, mean_send, mean_recv,
        device_id={"comp": 1 - comp}, device_id_type=MESH,
    )

    @pl.when(comp == 0)
    def _():
        depth = rows // 2
        turns = SUBCYCLES // depth
        clear_edges(turns)
        loads[0].wait()
        enter()
        pairs = [exchange_of(0, initial)]
        start(pairs[0])
        for copy in loads[1:]:
            copy.wait()
        covered = cover[...].astype(jnp.float32)
        push = covered / (inertia * forcing[0] + 1.0)
        own_stat[0] = forcing[1] * covered * (1.0 / 3.0)
        own_stat[1] = push
        own_stat[2] = push * (forcing[2] + current[0])
        own_stat[3] = push * (forcing[3] + current[1])
        stat_pair = stats_of(own_stat, 4)
        start(stat_pair)
        for turn in range(turns):
            source = initial if turn == 0 else own.at[turn - 1]
            if turn > 0:
                pairs.append(exchange_of(turn, source))
                start(pairs[turn])
            relay(pairs[turn])
            if turn == 0:
                relay(stat_pair)
                pl.semaphore_signal(
                    go, inc=1, device_id={"comp": 1 - comp}, device_id_type=MESH
                )
            fill_own(source)
            arrive(pairs[turn])
            if turn == 0:
                arrive(stat_pair)
                for place, block in enumerate((halo_stat.at[0], own_stat, halo_stat.at[1])):
                    span = slice(place * rows, (place + 1) * rows)
                    push = block[1]
                    stat[0, span] = block[0]
                    stat[1, span] = jnp.where(push > 0.0, 1.0 - push, 0.0)
                    stat[2, span] = 0.25 * push
                    stat[3, span] = block[2]
                    stat[4, span] = block[3]
            fill_sides(turn)

            def subcycle(step, carry):
                for chunk in range(chunks):
                    stress_stage(work, stat, chunk * width, width)
                for chunk in range(chunks):
                    velocity_stage(work, stat, total, chunk * width, width, rows)
                return carry

            lax.fori_loop(0, depth, subcycle, 0)
            final = state if turn == turns - 1 else own.at[turn]
            for field in range(fields):
                final[field] = work[field, rows : 2 * rows, inside]
        share = 1.0 / SUBCYCLES
        covered = cover[...].astype(jnp.float32)
        mean[0] = total[0] * share - covered * current[0]
        mean[1] = total[1] * share - covered * current[1]
        mean[2] = forcing[4] * covered * (total[2] * share)
        mean_copy.start()
        average[...] = mean[...]
        sent(stat_pair)
        for pair in pairs:
            sent(pair)
        mean_copy.wait_send()

    @pl.when(comp == 1)
    def _():
        depth = rows
        turns = SUBCYCLES // depth
        clear_edges(turns)
        spare[...] = jnp.zeros_like(spare)
        for copy in loads:
            copy.wait()
        enter()
        pl.semaphore_wait(go, 1)
        pairs = [exchange_of(0, initial)]
        start(pairs[0])
        stat_pair = stats_of(current, 2)
        start(stat_pair)
        for turn in range(turns):
            source = initial if turn == 0 else own.at[turn - 1]
            if turn > 0:
                pairs.append(exchange_of(turn, source))
                start(pairs[turn])
            relay(pairs[turn])
            if turn == 0:
                relay(stat_pair)
            fill_own(source)
            arrive(pairs[turn])
            if turn == 0:
                arrive(stat_pair)
                for place in range(3):
                    span = slice(place * rows, (place + 1) * rows)
                    for axis in range(2):
                        if place == 1:
                            speed = current[axis]
                        else:
                            speed = halo_stat[place // 2, axis]
                        stat[2 * axis, span] = courant * jnp.maximum(speed, 0.0)
                        stat[2 * axis + 1, span] = courant * jnp.minimum(speed, 0.0)
            fill_sides(turn)

            def substeps(step, carry):
                for chunk in range(chunks):
                    ocean_stage(work, spare, stat, chunk * width, width)
                for chunk in range(chunks):
                    ocean_stage(spare, work, stat, chunk * width, width)
                return carry

            lax.fori_loop(0, depth // 2, substeps, 0)
            final = state if turn == turns - 1 else own.at[turn]
            for field in range(fields):
                final[field] = work[field, rows : 2 * rows, inside]
        sent(stat_pair)
        for pair in pairs:
            sent(pair)
        mean_copy.wait_recv()


def run_turns(initial, forcing, current, cover):
    fields, rows, cols = initial.shape
    most = SUBCYCLES // (rows // 2)
    f32 = jnp.float32
    vmem = pl.BlockSpec(memory_space=pltpu.VMEM)
    dma = pltpu.SemaphoreType.DMA
    return pl.pallas_call(
        turns_kernel,
        out_shape=(
            jax.ShapeDtypeStruct((fields, rows, cols), f32),
            jax.ShapeDtypeStruct((3, rows, cols), f32),
        ),
        in_specs=[pl.BlockSpec(memory_space=pl.ANY)] * 4,
        out_specs=(vmem, vmem),
        scratch_shapes=[
            pltpu.VMEM(initial.shape, f32),
            pltpu.VMEM(forcing.shape, f32),
            pltpu.VMEM(current.shape, f32),
            pltpu.VMEM(cover.shape, cover.dtype),
            pltpu.VMEM((most, fields, rows, cols), f32),
            pltpu.VMEM((4, rows, cols), f32),
            pltpu.VMEM((most, 2, fields, rows, cols), f32),
            pltpu.VMEM((2, 4, rows, cols), f32),
            pltpu.VMEM((fields, 3 * rows, cols + 2 * PAD), f32),
            pltpu.VMEM((fields, 3 * rows, cols + 2 * PAD), f32),
            pltpu.VMEM((5, 3 * rows, cols), f32),
            pltpu.VMEM((3, rows, cols), f32),
            pltpu.VMEM((3, rows, cols), f32),
            dma((4,)),
            dma((most, fields)), dma((most, fields)), dma((most, fields)), dma((most, fields)),
            dma((4,)), dma((4,)), dma((4,)), dma((4,)),
            dma, dma, pltpu.SemaphoreType.REGULAR,
        ],
        compiler_params=pltpu.CompilerParams(
            collective_id=0, has_side_effects=True
        ),
        name="turns",
    )(initial, forcing, current, cover)


def remap_kernel(average, targets, weights, window, acc, low_index, high_index):
    comp = lax.axis_index("comp")
    channels, rows, cols = average.shape
    span = low_index.shape[1]
    low_count, high_count = low_index.shape[0], high_index.shape[0]
    bf16 = jnp.bfloat16
    blocks = cols // low_count
    low_index[...] = lax.broadcasted_iota(jnp.int32, low_index.shape, 0).astype(bf16)
    high_index[...] = lax.broadcasted_iota(jnp.int32, high_index.shape, 0).astype(bf16)
    acc[...] = jnp.zeros_like(acc)

    def one_row(row, carry):
        for piece in range(cols // span):
            place = pl.ds(piece * span, span)
            target = targets[comp, pl.ds(row, 1), place]
            scale = weights[comp, pl.ds(row, 1), place].astype(jnp.float32) * (1.0 / weight_norm)
            low = lax.rem(target, low_count)
            block = lax.rem(lax.div(target, low_count), blocks)
            line = lax.div(target, cols)
            high = (lax.div(line, rows) * blocks + block) * rows + lax.rem(line, rows)
            low_hot = jnp.where(low_index[...] == low.astype(bf16), bf16(1), bf16(0))
            match = high_index[...] == high.astype(bf16)
            parts = []
            for channel in range(channels):
                value = average[channel, pl.ds(row, 1), place] * scale
                coarse = value.astype(bf16)
                fine = (value - coarse.astype(jnp.float32)).astype(bf16)
                parts.append(jnp.where(match, coarse, bf16(0)))
                parts.append(jnp.where(match, fine, bf16(0)))
            spread = jnp.concatenate(parts, axis=0)
            acc[...] += lax.dot_general(
                spread, low_hot, (((1,), (1,)), ((), ())), preferred_element_type=jnp.float32
            )
        return carry

    lax.fori_loop(0, rows, one_row, 0)
    for channel in range(channels):
        for half in range(2):
            for block in range(blocks):
                base = 2 * channel * high_count + (half * blocks + block) * rows
                window[channel, half, :, block * low_count : (block + 1) * low_count] = (
                    acc[base : base + rows] + acc[base + high_count : base + high_count + rows]
                )


def run_remap(average, targets, weights):
    channels, rows, cols = average.shape
    low_count = 256 if cols % 256 == 0 else 128
    high_count = 2 * rows * cols // low_count
    span = min(1024, cols)
    vmem = pl.BlockSpec(memory_space=pltpu.VMEM)
    return pl.pallas_call(
        remap_kernel,
        out_shape=jax.ShapeDtypeStruct((channels, 2, rows, cols), jnp.float32),
        in_specs=[vmem] * 3,
        out_specs=vmem,
        scratch_shapes=[
            pltpu.VMEM((2 * channels * high_count, low_count), jnp.float32),
            pltpu.VMEM((low_count, span), jnp.bfloat16),
            pltpu.VMEM((high_count, span), jnp.bfloat16),
        ],
        compiler_params=pltpu.CompilerParams(vmem_limit_bytes=40 * 1024 * 1024),
        name="remap",
    )(average, targets, weights)


def join_kernel(
    window, state, average, out_state, out_pair, beside, carry, before,
    side_send, side_recv, next_send, next_recv,
):
    me = lax.axis_index("blk")
    comp = lax.axis_index("comp")
    count = lax.axis_size("blk")
    right, left = lax.rem(me + 1, count), lax.rem(me + count - 1, count)
    barrier = pltpu.get_barrier_semaphore()
    pl.semaphore_signal(barrier, inc=1, device_id={"blk": right}, device_id_type=MESH)
    pl.semaphore_signal(barrier, inc=1, device_id={"blk": left}, device_id_type=MESH)
    pl.semaphore_signal(barrier, inc=1, device_id={"comp": 1 - comp}, device_id_type=MESH)
    pl.semaphore_wait(barrier, 3)
    channels = window.shape[0]
    sides, onward = [], []
    for half in (1, 0):
        for channel in range(channels):
            sides.append(
                pltpu.make_async_remote_copy(
                    window.at[channel, half], beside.at[channel, half],
                    side_send.at[half, channel], side_recv.at[half, channel],
                    device_id={"comp": 1 - comp}, device_id_type=MESH,
                )
            )
    for channel in range(channels):
        onward.append(
            pltpu.make_async_remote_copy(
                carry.at[channel], before.at[channel],
                next_send.at[channel], next_recv.at[channel],
                device_id={"blk": right}, device_id_type=MESH,
            )
        )

    @pl.when(comp == 0)
    def _():
        for copy in sides:
            copy.start()
        out_state[...] = state[...]
        out_pair[...] = average[...]
        for copy in sides:
            copy.wait_send()

    @pl.when(comp == 1)
    def _():
        for channel in range(channels):
            sides[channel].wait_recv()
            carry[channel] = window[channel, 1] + beside[channel, 1]
            onward[channel].start()
        for channel in range(channels):
            sides[channels + channel].wait_recv()
            out_pair[channel] = window[channel, 0] + beside[channel, 0]
        out_state[...] = state[...]
        for channel in range(channels):
            onward[channel].wait_recv()
            out_pair[channel] += before[channel]
        out_state[0] -= dilution * out_pair[2]
        for channel in range(channels):
            onward[channel].wait_send()


def run_join(window, state, average):
    channels, rows, cols = average.shape
    vmem = pl.BlockSpec(memory_space=pltpu.VMEM)
    dma = pltpu.SemaphoreType.DMA
    return pl.pallas_call(
        join_kernel,
        out_shape=(
            jax.ShapeDtypeStruct(state.shape, jnp.float32),
            jax.ShapeDtypeStruct(average.shape, jnp.float32),
        ),
        in_specs=[vmem] * 3,
        out_specs=(vmem, vmem),
        scratch_shapes=[
            pltpu.VMEM(window.shape, jnp.float32),
            pltpu.VMEM(average.shape, jnp.float32),
            pltpu.VMEM(average.shape, jnp.float32),
            dma((2, channels)), dma((2, channels)), dma((channels,)), dma((channels,)),
        ],
        compiler_params=pltpu.CompilerParams(
            collective_id=1, has_side_effects=True, vmem_limit_bytes=40 * 1024 * 1024
        ),
        name="join",
    )(window, state, average)


def body(initial, ice_forcing, ocean_current, ice_cover, targets, weights):
    state, average = run_turns(initial[0], ice_forcing, ocean_current, ice_cover)
    window = run_remap(average, targets, weights)
    state, coupled = run_join(window, state, average)
    return (state[None], coupled[None])


def solution(mesh):
    placed = (
        P("comp", None, "blk", None),
        P(None, "blk", None),
        P(None, "blk", None),
        P("blk", None),
        P(None, "blk", None),
        P(None, "blk", None),
    )
    return jax.shard_map(
        body,
        mesh=mesh,
        in_specs=placed,
        out_specs=(P("comp", None, "blk", None), P("comp", None, "blk", None)),
        check_vma=False,
    )
```

```python
import functools

import jax
import jax.numpy as jnp
from jax import lax
from jax.experimental import pallas as pl
from jax.experimental.pallas import tpu as pltpu
from jax.sharding import PartitionSpec as P

SUBCYCLES = 16
MESH = pl.DeviceIdType.MESH
PAD = 128
PARTS = 2

coriolis = 0.1
inertia = 4.0
courant = 0.2
dilution = 0.5
weight_norm = 4.0
level_speed = (1.0, 0.8, 0.6, 0.45, 0.3)


def rolled(value, steps, axis):
    return pltpu.roll(value, steps % value.shape[axis], axis)


def rows_diff(value):
    return rolled(value, -1, 0) - rolled(value, 1, 0)


def chunk_width(cols):
    return 256 if cols % 256 == 0 else 128


def stress_stage(work, stat, start, width):
    wide = pl.ds(start, width + 2 * PAD)
    mid = pl.ds(start + PAD, width)
    inner = slice(PAD, PAD + width)
    vel_x, vel_y = work[0, :, wide], work[1, :, wide]
    cx = (rolled(vel_x, -1, 1) - rolled(vel_x, 1, 1))[:, inner]
    cy = (rolled(vel_y, -1, 1) - rolled(vel_y, 1, 1))[:, inner]
    rx = rows_diff(vel_x[:, inner])
    ry = rows_diff(vel_y[:, inner])
    e_d = rx + cy
    e_t = rx - cy
    e_s = cx + ry
    inv = lax.rsqrt(0.25 * (e_d * e_d) + 0.0625 * (e_t * e_t + e_s * e_s) + 0.01)
    third = stat[0, :, pl.ds(start, width)]
    scaled = third * inv
    work[2, :, mid] = work[2, :, mid] * (2.0 / 3.0) + (0.5 * scaled * e_d - third)
    work[3, :, mid] = work[3, :, mid] * (2.0 / 3.0) + 0.125 * scaled * e_t
    work[4, :, mid] = work[4, :, mid] * (2.0 / 3.0) + 0.0625 * scaled * e_s


def velocity_stage(work, stat, total, start, width, rows):
    wide = pl.ds(start, width + 2 * PAD)
    mid = pl.ds(start + PAD, width)
    here = pl.ds(start, width)
    inner = slice(PAD, PAD + width)
    shear = work[4, :, wide]
    one, two = work[2, :, wide], work[3, :, wide]
    across_shear = (rolled(shear, -1, 1) - rolled(shear, 1, 1))[:, inner]
    lower = one - two
    across_yy = (rolled(lower, -1, 1) - rolled(lower, 1, 1))[:, inner]
    force_x = rows_diff((one + two)[:, inner]) + 2.0 * across_shear
    force_y = 2.0 * rows_diff(shear[:, inner]) + across_yy
    old_x, old_y = work[0, :, mid], work[1, :, mid]
    keep, push = stat[1, :, here], stat[2, :, here]
    new_x = keep * (old_x + coriolis * old_y) + push * force_x + stat[3, :, here]
    new_y = keep * (old_y - coriolis * old_x) + push * force_y + stat[4, :, here]
    work[0, :, mid] = new_x
    work[1, :, mid] = new_y
    own_x, own_y = new_x[rows : 2 * rows], new_y[rows : 2 * rows]
    total[0, :, here] += own_x
    total[1, :, here] += own_y
    total[2, :, here] += jnp.sqrt(1.0 + own_x * own_x + own_y * own_y)


def ocean_stage(source, target, coef, start, width):
    wide = pl.ds(start, width + 2 * PAD)
    mid = pl.ds(start + PAD, width)
    here = pl.ds(start, width)
    inner = slice(PAD, PAD + width)
    up, down, east, west = (coef[i, :, here] for i in range(4))
    for level, speed in enumerate(level_speed):
        tracer = source[level, :, wide]
        centre = tracer[:, inner]
        right = rolled(tracer, -1, 1)[:, inner] - centre
        left = centre - rolled(tracer, 1, 1)[:, inner]
        above = rolled(centre, -1, 0) - centre
        below = centre - rolled(centre, 1, 0)
        change = up * below + down * above + east * left + west * right
        target[level, :, mid] = centre - speed * change


def turns_kernel(
    initial_in, forcing_in, current_in, cover_in, state, average,
    initial, forcing, current, cover,
    own, own_stat, halo, halo_stat, work, spare, stat, total, mean,
    load, near_send, near_recv, far_send, far_recv,
    stat_near_send, stat_near_recv, stat_far_send, stat_far_recv,
    mean_send, mean_recv, go,
):
    me = lax.axis_index("blk")
    comp = lax.axis_index("comp")
    count = lax.axis_size("blk")
    fields, rows, cols = initial.shape
    width = chunk_width(cols)
    chunks = cols // width
    near = 1 - lax.rem(me, 2)
    far = 1 - near
    partner = me + 2 * near - 1
    relay_to = me + 4 * near - 2
    relay_from = me - 4 * near + 2
    can_send = jnp.logical_and(relay_to >= 0, relay_to < count)
    can_recv = jnp.logical_and(relay_from >= 0, relay_from < count)
    relay_to = lax.rem(relay_to + count, count)
    relay_from = lax.rem(relay_from + count, count)

    barrier = pltpu.get_barrier_semaphore()

    def greet(where):
        pl.semaphore_signal(barrier, inc=1, device_id=where, device_id_type=MESH)

    greet({"blk": partner})
    greet({"comp": 1 - comp})
    pl.when(can_send)(lambda: greet({"blk": relay_to}))
    pl.when(can_recv)(lambda: greet({"blk": relay_from}))
    loads = [
        pltpu.make_async_copy(source, target, load.at[i])
        for i, (source, target) in enumerate(
            (
                (initial_in, initial),
                (current_in, current),
                (forcing_in, forcing),
                (cover_in, cover),
            )
        )
    ]
    for copy in loads:
        copy.start()

    work[...] = jnp.zeros_like(work)
    total[...] = jnp.zeros_like(total)

    def enter():
        pl.semaphore_wait(barrier, 2 + can_send.astype(jnp.int32) + can_recv.astype(jnp.int32))

    def copies(source, target, pieces, near_sems, far_sems):
        first, second = [], []
        wide = cols // PARTS
        for index in range(pieces * PARTS):
            piece, place = index // PARTS, pl.ds(index % PARTS * wide, wide)
            first.append(
                pltpu.make_async_remote_copy(
                    source.at[piece, :, place], target.at[far, piece, :, place],
                    near_sems[0].at[index], near_sems[1].at[index],
                    device_id={"blk": partner}, device_id_type=MESH,
                )
            )
            second.append(
                pltpu.make_async_remote_copy(
                    target.at[near, piece, :, place], target.at[far, piece, :, place],
                    far_sems[0].at[index], far_sems[1].at[index],
                    device_id={"blk": relay_to}, device_id_type=MESH,
                )
            )
        return first, second

    def start(pair):
        for copy in pair[0]:
            copy.start()

    def relay(pair):
        for first, second in zip(*pair):
            first.wait_recv()
            pl.when(can_send)(second.start)

    def arrive(pair):
        @pl.when(can_recv)
        def _():
            for copy in pair[1]:
                copy.wait_recv()

    def sent(pair):
        for copy in pair[0]:
            copy.wait_send()

        @pl.when(can_send)
        def _():
            for copy in pair[1]:
                copy.wait_send()

    def clear_edges(turns):
        @pl.when(jnp.logical_not(can_recv))
        def _():
            halo_stat[far] = jnp.zeros(halo_stat.shape[1:], jnp.float32)
            for turn in range(turns):
                halo[turn, far] = jnp.zeros(halo.shape[2:], jnp.float32)

    inside = slice(PAD, PAD + cols)

    def fill_own(source):
        for field in range(fields):
            work[field, rows : 2 * rows, inside] = source[field]

    def fill_sides(turn):
        for field in range(fields):
            work[field, 0:rows, inside] = halo[turn, 0, field]
            work[field, 2 * rows : 3 * rows, inside] = halo[turn, 1, field]

    def exchange_of(turn, source):
        return copies(
            source, halo.at[turn], fields,
            (near_send.at[turn], near_recv.at[turn]), (far_send.at[turn], far_recv.at[turn]),
        )

    def stats_of(source, pieces):
        return copies(
            source, halo_stat, pieces,
            (stat_near_send, stat_near_recv), (stat_far_send, stat_far_recv),
        )

    mean_copy = pltpu.make_async_remote_copy(
        mean, average, mean_send, mean_recv,
        device_id={"comp": 1 - comp}, device_id_type=MESH,
    )

    @pl.when(comp == 0)
    def _():
        depth = rows // 2
        turns = SUBCYCLES // depth
        clear_edges(turns)
        loads[0].wait()
        enter()
        pairs = [exchange_of(0, initial)]
        start(pairs[0])
        for copy in loads[1:]:
            copy.wait()
        covered = cover[...].astype(jnp.float32)
        push = covered / (inertia * forcing[0] + 1.0)
        own_stat[0] = forcing[1] * covered * (1.0 / 3.0)
        own_stat[1] = push
        own_stat[2] = push * (forcing[2] + current[0])
        own_stat[3] = push * (forcing[3] + current[1])
        stat_pair = stats_of(own_stat, 4)
        start(stat_pair)
        for turn in range(turns):
            source = initial if turn == 0 else own.at[turn - 1]
            if turn > 0:
                pairs.append(exchange_of(turn, source))
                start(pairs[turn])
            relay(pairs[turn])
            if turn == 0:
                relay(stat_pair)
                pl.semaphore_signal(
                    go, inc=1, device_id={"comp": 1 - comp}, device_id_type=MESH
                )
            fill_own(source)
            arrive(pairs[turn])
            if turn == 0:
                arrive(stat_pair)
                for place, block in enumerate((halo_stat.at[0], own_stat, halo_stat.at[1])):
                    span = slice(place * rows, (place + 1) * rows)
                    push = block[1]
                    stat[0, span] = block[0]
                    stat[1, span] = jnp.where(push > 0.0, 1.0 - push, 0.0)
                    stat[2, span] = 0.25 * push
                    stat[3, span] = block[2]
                    stat[4, span] = block[3]
            fill_sides(turn)

            def subcycle(step, carry):
                for chunk in range(chunks):
                    stress_stage(work, stat, chunk * width, width)
                for chunk in range(chunks):
                    velocity_stage(work, stat, total, chunk * width, width, rows)
                return carry

            lax.fori_loop(0, depth, subcycle, 0)
            final = state if turn == turns - 1 else own.at[turn]
            for field in range(fields):
                final[field] = work[field, rows : 2 * rows, inside]
        share = 1.0 / SUBCYCLES
        covered = cover[...].astype(jnp.float32)
        mean[0] = total[0] * share - covered * current[0]
        mean[1] = total[1] * share - covered * current[1]
        mean[2] = forcing[4] * covered * (total[2] * share)
        mean_copy.start()
        average[...] = mean[...]
        sent(stat_pair)
        for pair in pairs:
            sent(pair)
        mean_copy.wait_send()

    @pl.when(comp == 1)
    def _():
        depth = rows
        turns = SUBCYCLES // depth
        clear_edges(turns)
        spare[...] = jnp.zeros_like(spare)
        for copy in loads:
            copy.wait()
        enter()
        pl.semaphore_wait(go, 1)
        pairs = [exchange_of(0, initial)]
        start(pairs[0])
        stat_pair = stats_of(current, 2)
        start(stat_pair)
        for turn in range(turns):
            source = initial if turn == 0 else own.at[turn - 1]
            if turn > 0:
                pairs.append(exchange_of(turn, source))
                start(pairs[turn])
            relay(pairs[turn])
            if turn == 0:
                relay(stat_pair)
            fill_own(source)
            arrive(pairs[turn])
            if turn == 0:
                arrive(stat_pair)
                for place in range(3):
                    span = slice(place * rows, (place + 1) * rows)
                    for axis in range(2):
                        if place == 1:
                            speed = current[axis]
                        else:
                            speed = halo_stat[place // 2, axis]
                        stat[2 * axis, span] = courant * jnp.maximum(speed, 0.0)
                        stat[2 * axis + 1, span] = courant * jnp.minimum(speed, 0.0)
            fill_sides(turn)

            def substeps(step, carry):
                for chunk in range(chunks):
                    ocean_stage(work, spare, stat, chunk * width, width)
                for chunk in range(chunks):
                    ocean_stage(spare, work, stat, chunk * width, width)
                return carry

            lax.fori_loop(0, depth // 2, substeps, 0)
            final = state if turn == turns - 1 else own.at[turn]
            for field in range(fields):
                final[field] = work[field, rows : 2 * rows, inside]
        sent(stat_pair)
        for pair in pairs:
            sent(pair)
        mean_copy.wait_recv()


def run_turns(initial, forcing, current, cover):
    fields, rows, cols = initial.shape
    most = SUBCYCLES // (rows // 2)
    f32 = jnp.float32
    vmem = pl.BlockSpec(memory_space=pltpu.VMEM)
    dma = pltpu.SemaphoreType.DMA
    return pl.pallas_call(
        turns_kernel,
        out_shape=(
            jax.ShapeDtypeStruct((fields, rows, cols), f32),
            jax.ShapeDtypeStruct((3, rows, cols), f32),
        ),
        in_specs=[pl.BlockSpec(memory_space=pl.ANY)] * 4,
        out_specs=(vmem, vmem),
        scratch_shapes=[
            pltpu.VMEM(initial.shape, f32),
            pltpu.VMEM(forcing.shape, f32),
            pltpu.VMEM(current.shape, f32),
            pltpu.VMEM(cover.shape, cover.dtype),
            pltpu.VMEM((most, fields, rows, cols), f32),
            pltpu.VMEM((4, rows, cols), f32),
            pltpu.VMEM((most, 2, fields, rows, cols), f32),
            pltpu.VMEM((2, 4, rows, cols), f32),
            pltpu.VMEM((fields, 3 * rows, cols + 2 * PAD), f32),
            pltpu.VMEM((fields, 3 * rows, cols + 2 * PAD), f32),
            pltpu.VMEM((5, 3 * rows, cols), f32),
            pltpu.VMEM((3, rows, cols), f32),
            pltpu.VMEM((3, rows, cols), f32),
            dma((4,)),
            *[dma((most, fields * PARTS)) for _ in range(4)],
            *[dma((4 * PARTS,)) for _ in range(4)],
            dma, dma, pltpu.SemaphoreType.REGULAR,
        ],
        compiler_params=pltpu.CompilerParams(
            collective_id=0, has_side_effects=True
        ),
        name="turns",
    )(initial, forcing, current, cover)


def remap_kernel(average, targets, weights, window, acc, low_index, high_index):
    comp = lax.axis_index("comp")
    channels, rows, cols = average.shape
    span = low_index.shape[1]
    low_count, high_count = low_index.shape[0], high_index.shape[0]
    bf16 = jnp.bfloat16
    blocks = cols // low_count
    low_index[...] = lax.broadcasted_iota(jnp.int32, low_index.shape, 0).astype(bf16)
    high_index[...] = lax.broadcasted_iota(jnp.int32, high_index.shape, 0).astype(bf16)
    acc[...] = jnp.zeros_like(acc)

    def one_row(row, carry):
        for piece in range(cols // span):
            place = pl.ds(piece * span, span)
            target = targets[comp, pl.ds(row, 1), place]
            scale = weights[comp, pl.ds(row, 1), place].astype(jnp.float32) * (1.0 / weight_norm)
            low = lax.rem(target, low_count)
            block = lax.rem(lax.div(target, low_count), blocks)
            line = lax.div(target, cols)
            high = (lax.div(line, rows) * blocks + block) * rows + lax.rem(line, rows)
            low_hot = jnp.where(low_index[...] == low.astype(bf16), bf16(1), bf16(0))
            match = high_index[...] == high.astype(bf16)
            parts = []
            for channel in range(channels):
                value = average[channel, pl.ds(row, 1), place] * scale
                coarse = value.astype(bf16)
                fine = (value - coarse.astype(jnp.float32)).astype(bf16)
                parts.append(jnp.where(match, coarse, bf16(0)))
                parts.append(jnp.where(match, fine, bf16(0)))
            spread = jnp.concatenate(parts, axis=0)
            acc[...] += lax.dot_general(
                spread, low_hot, (((1,), (1,)), ((), ())), preferred_element_type=jnp.float32
            )
        return carry

    lax.fori_loop(0, rows, one_row, 0)
    for channel in range(channels):
        for half in range(2):
            for block in range(blocks):
                base = 2 * channel * high_count + (half * blocks + block) * rows
                window[channel, half, :, block * low_count : (block + 1) * low_count] = (
                    acc[base : base + rows] + acc[base + high_count : base + high_count + rows]
                )


def run_remap(average, targets, weights):
    channels, rows, cols = average.shape
    low_count = 256 if cols % 256 == 0 else 128
    high_count = 2 * rows * cols // low_count
    span = min(1024, cols)
    vmem = pl.BlockSpec(memory_space=pltpu.VMEM)
    return pl.pallas_call(
        remap_kernel,
        out_shape=jax.ShapeDtypeStruct((channels, 2, rows, cols), jnp.float32),
        in_specs=[vmem] * 3,
        out_specs=vmem,
        scratch_shapes=[
            pltpu.VMEM((2 * channels * high_count, low_count), jnp.float32),
            pltpu.VMEM((low_count, span), jnp.bfloat16),
            pltpu.VMEM((high_count, span), jnp.bfloat16),
        ],
        compiler_params=pltpu.CompilerParams(vmem_limit_bytes=40 * 1024 * 1024),
        name="remap",
    )(average, targets, weights)


def join_kernel(
    window, state, average, out_state, out_pair, beside, carry, before,
    side_send, side_recv, next_send, next_recv,
):
    me = lax.axis_index("blk")
    comp = lax.axis_index("comp")
    count = lax.axis_size("blk")
    right, left = lax.rem(me + 1, count), lax.rem(me + count - 1, count)
    barrier = pltpu.get_barrier_semaphore()
    pl.semaphore_signal(barrier, inc=1, device_id={"blk": right}, device_id_type=MESH)
    pl.semaphore_signal(barrier, inc=1, device_id={"blk": left}, device_id_type=MESH)
    pl.semaphore_signal(barrier, inc=1, device_id={"comp": 1 - comp}, device_id_type=MESH)
    pl.semaphore_wait(barrier, 3)
    channels = window.shape[0]
    sides, onward = [], []
    for half in (1, 0):
        for channel in range(channels):
            sides.append(
                pltpu.make_async_remote_copy(
                    window.at[channel, half], beside.at[channel, half],
                    side_send.at[half, channel], side_recv.at[half, channel],
                    device_id={"comp": 1 - comp}, device_id_type=MESH,
                )
            )
    for channel in range(channels):
        onward.append(
            pltpu.make_async_remote_copy(
                carry.at[channel], before.at[channel],
                next_send.at[channel], next_recv.at[channel],
                device_id={"blk": right}, device_id_type=MESH,
            )
        )

    @pl.when(comp == 0)
    def _():
        for copy in sides:
            copy.start()
        out_state[...] = state[...]
        out_pair[...] = average[...]
        for copy in sides:
            copy.wait_send()

    @pl.when(comp == 1)
    def _():
        for channel in range(channels):
            sides[channel].wait_recv()
            carry[channel] = window[channel, 1] + beside[channel, 1]
            onward[channel].start()
        for channel in range(channels):
            sides[channels + channel].wait_recv()
            out_pair[channel] = window[channel, 0] + beside[channel, 0]
        out_state[...] = state[...]
        for channel in range(channels):
            onward[channel].wait_recv()
            out_pair[channel] += before[channel]
        out_state[0] -= dilution * out_pair[2]
        for channel in range(channels):
            onward[channel].wait_send()


def run_join(window, state, average):
    channels, rows, cols = average.shape
    vmem = pl.BlockSpec(memory_space=pltpu.VMEM)
    dma = pltpu.SemaphoreType.DMA
    return pl.pallas_call(
        join_kernel,
        out_shape=(
            jax.ShapeDtypeStruct(state.shape, jnp.float32),
            jax.ShapeDtypeStruct(average.shape, jnp.float32),
        ),
        in_specs=[vmem] * 3,
        out_specs=(vmem, vmem),
        scratch_shapes=[
            pltpu.VMEM(window.shape, jnp.float32),
            pltpu.VMEM(average.shape, jnp.float32),
            pltpu.VMEM(average.shape, jnp.float32),
            dma((2, channels)), dma((2, channels)), dma((channels,)), dma((channels,)),
        ],
        compiler_params=pltpu.CompilerParams(
            collective_id=1, has_side_effects=True, vmem_limit_bytes=40 * 1024 * 1024
        ),
        name="join",
    )(window, state, average)


def body(initial, ice_forcing, ocean_current, ice_cover, targets, weights):
    state, average = run_turns(initial[0], ice_forcing, ocean_current, ice_cover)
    window = run_remap(average, targets, weights)
    state, coupled = run_join(window, state, average)
    return (state[None], coupled[None])


def solution(mesh):
    placed = (
        P("comp", None, "blk", None),
        P(None, "blk", None),
        P(None, "blk", None),
        P("blk", None),
        P(None, "blk", None),
        P(None, "blk", None),
    )
    return jax.shard_map(
        body,
        mesh=mesh,
        in_specs=placed,
        out_specs=(P("comp", None, "blk", None), P("comp", None, "blk", None)),
        check_vma=False,
    )
```
